32 devices in a mesh: files: 8 (over z, y), rep: 4 (over x, core).
Axes of the slice: x: 2, y: 2, z: 4, core: 2. Of those that a mesh axis runs over, the one named last changes fastest.
Arguments:
- tile_id: int32 [131072], P(('files', 'rep')), may hold values from 0 to 127, as said below
- pix_row: int32 [131072], P(('files', 'rep')), may hold values from 0 to 31
- pix_col: int32 [131072], P(('files', 'rep')), may hold values from 0 to 127
- point_value: bfloat16 [131072], P(('files', 'rep')), may hold values from -6 to 6
Outputs:
- tile_sums: float32 [128, 32, 128], P('files', 'rep')
The draws below stay inside these ranges and needn't reach their ends.
Inputs may be any that keep to these rules, and one draw needn't show every extreme that they name: `tile_id`: of the points of one device, at most 2048 lie in tiles of one file group (tile id modulo 8), and on every device some group holds exactly 2048 of them.
All inputs are finite; a program needn't handle non-finite values.
Results may differ from the reference program's by a relative error of at most 0.0003.
Values sent between devices are 32-bit elements; how exact they have to be, the bound alone decides.
A program may use at most 64 MiB of HBM per device.

```python
import jax
import jax.numpy as jnp

TC = 128
TR = 32
PTS_DEV = 4096
TILES = 128
TILE_OWN = 16
CAP = 2048
POINTS = 131072
N_FILES = 8
N_REP = 4


def draw_tile_id(key, part):
    device_count = POINTS // PTS_DEV
    tier_most = N_FILES // 8
    middle_low = max(1, CAP // 4)
    middle_high = max(middle_low, CAP // 2)

    def one_device(device_key):
        key_order = jax.random.fold_in(device_key, 1)
        key_local = jax.random.fold_in(device_key, 2)
        key_mixing = jax.random.fold_in(device_key, 3)
        key_heavy = jax.random.fold_in(device_key, 4)
        key_middle = jax.random.fold_in(device_key, 5)
        key_size = jax.random.fold_in(device_key, 6)
        owner_order = jax.random.permutation(key_order, N_FILES)
        heavy_count = jax.random.randint(key_heavy, (), 1, tier_most + 1)
        middle_count = jax.random.randint(key_middle, (), 0, tier_most + 1)
        middle_size = jax.random.randint(key_size, (), middle_low, middle_high + 1)
        slot_index = jnp.arange(PTS_DEV, dtype=jnp.int32)
        heavy_end = heavy_count * CAP
        middle_end = heavy_end + middle_count * middle_size
        rest_owners = N_FILES - heavy_count - middle_count
        rank_heavy = slot_index // CAP
        rank_middle = heavy_count + (slot_index - heavy_end) // middle_size
        rank_rest = heavy_count + middle_count + (slot_index - middle_end) % rest_owners
        pick_rank = jnp.where(slot_index < heavy_end, rank_heavy, jnp.where(slot_index < middle_end, rank_middle, rank_rest))
        pick_rank = jnp.clip(pick_rank, 0, N_FILES - 1).astype(jnp.int32)
        tile_owner = owner_order[pick_rank]
        tile_local = jax.random.randint(key_local, (PTS_DEV,), 0, TILE_OWN)
        tile_ids = tile_owner + N_FILES * tile_local
        return jax.random.permutation(key_mixing, tile_ids)
    device_keys = jax.random.split(jax.random.fold_in(key, 11), device_count)
    return jax.vmap(one_device)(device_keys).reshape(POINTS).astype(jnp.int32)


def draw_pix_row(key, part):
    device_count = POINTS // PTS_DEV
    quarter = TR // N_REP

    def one_device(device_key):
        hot_quarter = jax.random.randint(jax.random.fold_in(device_key, 1), (), 0, N_REP)
        hot_share = jax.random.randint(jax.random.fold_in(device_key, 2), (), 3, 8)
        pick_tenth = jax.random.randint(jax.random.fold_in(device_key, 3), (PTS_DEV,), 0, 10)
        inner_row = jax.random.randint(jax.random.fold_in(device_key, 4), (PTS_DEV,), 0, quarter)
        spread_row = jax.random.randint(jax.random.fold_in(device_key, 5), (PTS_DEV,), 0, TR)
        return jnp.where(pick_tenth < hot_share, hot_quarter * quarter + inner_row, spread_row)
    device_keys = jax.random.split(jax.random.fold_in(key, 21), device_count)
    return jax.vmap(one_device)(device_keys).reshape(POINTS).astype(jnp.int32)


def with_ends(values, stream_key, smallest, top_value):
    extent = values.shape
    index_at = [jax.random.randint(jax.random.fold_in(stream_key, axis), (), 0, extent[axis]) for axis in range(len(extent))]
    values = values.at[tuple(index_at)].set(smallest)
    longest = extent.index(max(extent))
    index_at[longest] = (index_at[longest] + 1) % extent[longest]
    return values.at[tuple(index_at)].set(top_value)


def levels(own_key, shape, shards, least, largest):
    loudness = 1.0
    for dim, blocks in shards:
        draws = jax.random.uniform(jax.random.fold_in(jax.random.fold_in(own_key, 6), dim), (blocks,), jnp.float32, least / len(shards), largest / len(shards))
        loudness = loudness * jnp.repeat(jnp.exp(draws), shape[dim] // blocks).reshape((-1,) + (1,) * (len(shape) - 1 - dim))
    return loudness


def centred(key, shape, scale, limit, shards=(), kind=jnp.bfloat16):
    result = jax.random.normal(key, shape, jnp.float32) * scale
    if len(shards) > 0:
        result = levels(key, shape, shards, -0.22, 0.18) * result
    return jnp.clip(result, min=-limit, max=limit).astype(kind)


def setup_inputs(seed: int = 0) -> dict:
    keys = jax.random.split(jax.random.key(seed), 5)
    return {
        "tile_id": draw_tile_id(jax.random.fold_in(keys[4], 71), 0),
        "pix_row": draw_pix_row(jax.random.fold_in(keys[4], 71), 0),
        "pix_col": with_ends(jax.random.randint(keys[2], (POINTS,), 0, TC), jax.random.fold_in(keys[2], 1), 0, TC - 1).astype(jnp.int32),
        "point_value": centred(keys[3], (POINTS,), 1.0, 6.0, ((0, 32),)),
    }


def reference(tile_id, pix_row, pix_col, point_value):
    tile_owner = tile_id % N_FILES
    tile_local = tile_id // N_FILES
    owned_slot = tile_owner * TILE_OWN + tile_local
    flat_cell = (owned_slot * TR + pix_row) * TC + pix_col
    summed = jax.ops.segment_sum(point_value.astype(jnp.float32), flat_cell.astype(jnp.int32), num_segments=TILES * TR * TC)
    return summed.reshape(TILES, TR, TC)
```

```python
import functools

import jax
import jax.numpy as jnp
from jax import lax
from jax.experimental import pallas as pl
from jax.experimental.pallas import tpu as pltpu
from jax.sharding import PartitionSpec as P

LANES = 128
WIDE = 256
TR = 32
TILES = 128
ORDER = (1, 2, 6, 3, 7, 4, 5)
MESH = pl.DeviceIdType.MESH


def flipped(index, mask, count):
    out = index
    bit = 1
    while bit < count:
        if mask & bit:
            out = out + (1 - 2 * ((index // bit) % 2)) * bit
        bit *= 2
    return out


def kernel(nf, nr, owned, quarter, tile_ref, row_ref, col_ref, val_ref, parts,
           tile_in, row_in, col_in, val_in, got, acc,
           isem, osem, gsend, grecv, rsend, rrecv):
    f = lax.axis_index("files")
    r = lax.axis_index("rep")
    half = owned * quarter // 2
    band = nr * half
    blocks = tile_ref.shape[0]

    loads = []
    for i, (src, dst) in enumerate(((tile_ref, tile_in), (row_ref, row_in), (col_ref, col_in), (val_ref, val_in))):
        load = pltpu.make_async_copy(src, dst, isem.at[i])
        load.start()
        loads.append(load)
    barrier = pltpu.get_barrier_semaphore()
    for k in range(1, nf):
        pl.semaphore_signal(barrier, inc=1, device_id={"files": flipped(f, k, nf)}, device_id_type=MESH)
    for k in range(1, nr):
        pl.semaphore_signal(barrier, inc=1, device_id={"rep": flipped(r, k, nr)}, device_id_type=MESH)

    for load in loads:
        load.wait()
    tile = tile_in[...]
    prow = row_in[...]
    owner = tile % nf
    inner = (tile // nf) * quarter + prow % quarter
    cell = (owner * band + (prow // quarter) * half + inner % half) * WIDE
    cell = cell + (inner // half) * LANES + col_in[...]
    got[0, 0:blocks, :] = cell.astype(jnp.float32)
    got[0, blocks:, :] = val_in[...].astype(jnp.float32)

    pl.semaphore_wait(barrier, nf + nr - 2)

    sends = []
    for i, k in enumerate(ORDER if nf == 8 else range(1, nf), 1):
        copy = pltpu.make_async_remote_copy(
            src_ref=got.at[0], dst_ref=got.at[i], send_sem=gsend.at[i], recv_sem=grecv.at[i],
            device_id={"files": flipped(f, k, nf)}, device_id_type=MESH)
        copy.start()
        sends.append(copy)

    ids = [(lax.broadcasted_iota(jnp.int32, (16, LANES), 0) + 16 * i).astype(jnp.float32).astype(jnp.bfloat16)
           for i in range(WIDE // 16)]
    one = jnp.ones((), jnp.bfloat16)
    zero = jnp.zeros((), jnp.bfloat16)
    first = (f * band).astype(jnp.float32)

    def wide(line):
        return jnp.broadcast_to(line, (16, LANES)).astype(jnp.bfloat16)

    def add_points(cells, values):
        row = jnp.floor(cells * (1.0 / WIDE))
        col = cells - row * WIDE
        row = row - first
        lhs = []
        rhs = []
        for j in range(blocks):
            row16 = wide(row[j:j + 1, :])
            col16 = wide(col[j:j + 1, :])
            val16 = wide(values[j:j + 1, :])
            lhs.append(jnp.concatenate([jnp.where(row16 == ids[i], val16, zero) for i in range(band // 16)], axis=0))
            rhs.append(jnp.concatenate([jnp.where(col16 == ids[i], one, zero) for i in range(WIDE // 16)], axis=0))
        total = lax.dot_general(jnp.concatenate(lhs, axis=1), jnp.concatenate(rhs, axis=1),
                                (((1,), (1,)), ((), ())), preferred_element_type=jnp.float32)
        for q in range(nr):
            block = total[q * half:(q + 1) * half, :]
            acc[q, 0] += block[:, :LANES]
            acc[q, 1] += block[:, LANES:]

    acc[...] = jnp.zeros_like(acc)

    def wait_for(i):
        pltpu.make_async_remote_copy(
            src_ref=got.at[0], dst_ref=got.at[i], send_sem=gsend.at[i], recv_sem=grecv.at[i],
            device_id={"files": (f + 1) % nf}, device_id_type=MESH).wait_recv()

    def step(t, carry):
        pl.when(t > 0)(lambda: wait_for(t))
        add_points(got[t, 0:blocks, :], got[t, blocks:, :])
        return carry

    lax.fori_loop(0, nf, step, 0)

    backs = []
    for k in tuple(range(2, nr)) + (1,):
        peer = flipped(r, k, nr)
        copy = pltpu.make_async_remote_copy(
            src_ref=acc.at[peer], dst_ref=parts.at[k], send_sem=rsend.at[k], recv_sem=rrecv.at[k],
            device_id={"rep": peer}, device_id_type=MESH)
        copy.start()
        backs.append(copy)
    own = pltpu.make_async_copy(acc.at[r], parts.at[0], osem)
    own.start()
    for copy in sends:
        copy.wait_send()
    own.wait()
    for copy in backs:
        copy.wait()


def solution(mesh):
    nf = mesh.shape["files"]
    nr = mesh.shape["rep"]
    owned = TILES // nf
    quarter = TR // nr
    half = owned * quarter // 2

    def per_device(tile_id, pix_row, pix_col, point_value):
        blocks = tile_id.shape[0] // LANES
        shape = (blocks, LANES)
        out = pl.pallas_call(
            functools.partial(kernel, nf, nr, owned, quarter),
            out_shape=jax.ShapeDtypeStruct((nr, 2, half, LANES), jnp.float32),
            in_specs=[pl.BlockSpec(memory_space=pl.ANY)] * 4,
            out_specs=pl.BlockSpec(memory_space=pl.ANY),
            scratch_shapes=[
                pltpu.VMEM(shape, jnp.int32),
                pltpu.VMEM(shape, jnp.int32),
                pltpu.VMEM(shape, jnp.int32),
                pltpu.VMEM(shape, point_value.dtype),
                pltpu.VMEM((nf, 2 * blocks, LANES), jnp.float32),
                pltpu.VMEM((nr, 2, half, LANES), jnp.float32),
                pltpu.SemaphoreType.DMA((4,)),
                pltpu.SemaphoreType.DMA,
                pltpu.SemaphoreType.DMA((nf,)),
                pltpu.SemaphoreType.DMA((nf,)),
                pltpu.SemaphoreType.DMA((nr,)),
                pltpu.SemaphoreType.DMA((nr,)),
            ],
            compiler_params=pltpu.CompilerParams(collective_id=0, has_side_effects=True),
        )(tile_id.reshape(shape), pix_row.reshape(shape), pix_col.reshape(shape),
          point_value.reshape(shape))
        return jnp.sum(out, axis=0).reshape(owned, quarter, LANES)

    both = P(("files", "rep"))
    return jax.shard_map(per_device, mesh=mesh, in_specs=(both,) * 4,
                         out_specs=P("files", "rep", None), check_vma=False)
```

```python
import functools

import jax
import jax.numpy as jnp
from jax import lax
from jax.experimental import pallas as pl
from jax.experimental.pallas import tpu as pltpu
from jax.sharding import PartitionSpec as P

LANES = 128
WIDE = 256
TR = 32
TILES = 128
ORDER = (1, 2, 6, 3, 7, 4, 5)
MESH = pl.DeviceIdType.MESH


def flipped(index, mask, count):
    out = index
    bit = 1
    while bit < count:
        if mask & bit:
            out = out + (1 - 2 * ((index // bit) % 2)) * bit
        bit *= 2
    return out


def kernel(nf, nr, owned, quarter, tile_ref, row_ref, col_ref, val_ref, out,
           tile_in, row_in, col_in, val_in, got, acc, parts,
           isem, osem, gsend, grecv, rsend, rrecv):
    f = lax.axis_index("files")
    r = lax.axis_index("rep")
    half = owned * quarter // 2
    band = nr * half
    blocks = tile_ref.shape[0]

    loads = []
    for i, (src, dst) in enumerate(((tile_ref, tile_in), (row_ref, row_in), (col_ref, col_in), (val_ref, val_in))):
        load = pltpu.make_async_copy(src, dst, isem.at[i])
        load.start()
        loads.append(load)
    barrier = pltpu.get_barrier_semaphore()
    for k in range(1, nf):
        pl.semaphore_signal(barrier, inc=1, device_id={"files": flipped(f, k, nf)}, device_id_type=MESH)
    for k in range(1, nr):
        pl.semaphore_signal(barrier, inc=1, device_id={"rep": flipped(r, k, nr)}, device_id_type=MESH)

    for load in loads:
        load.wait()
    tile = tile_in[...]
    prow = row_in[...]
    owner = tile % nf
    inner = (tile // nf) * quarter + prow % quarter
    cell = (owner * band + (prow // quarter) * half + inner % half) * WIDE
    cell = cell + (inner // half) * LANES + col_in[...]
    got[0, 0:blocks, :] = cell.astype(jnp.float32)
    got[0, blocks:, :] = val_in[...].astype(jnp.float32)

    pl.semaphore_wait(barrier, nf + nr - 2)

    sends = []
    for i, k in enumerate(ORDER if nf == 8 else range(1, nf), 1):
        copy = pltpu.make_async_remote_copy(
            src_ref=got.at[0], dst_ref=got.at[i], send_sem=gsend.at[i], recv_sem=grecv.at[i],
            device_id={"files": flipped(f, k, nf)}, device_id_type=MESH)
        copy.start()
        sends.append(copy)

    ids = [(lax.broadcasted_iota(jnp.int32, (16, LANES), 0) + 16 * i).astype(jnp.float32).astype(jnp.bfloat16)
           for i in range(WIDE // 16)]
    one = jnp.ones((), jnp.bfloat16)
    zero = jnp.zeros((), jnp.bfloat16)
    first = (f * band).astype(jnp.float32)

    def wide(line):
        return jnp.broadcast_to(line, (16, LANES)).astype(jnp.bfloat16)

    def add_points(cells, values):
        row = jnp.floor(cells * (1.0 / WIDE))
        col = cells - row * WIDE
        row = row - first
        lhs = []
        rhs = []
        for j in range(blocks):
            row16 = wide(row[j:j + 1, :])
            col16 = wide(col[j:j + 1, :])
            val16 = wide(values[j:j + 1, :])
            lhs.append(jnp.concatenate([jnp.where(row16 == ids[i], val16, zero) for i in range(band // 16)], axis=0))
            rhs.append(jnp.concatenate([jnp.where(col16 == ids[i], one, zero) for i in range(WIDE // 16)], axis=0))
        total = lax.dot_general(jnp.concatenate(lhs, axis=1), jnp.concatenate(rhs, axis=1),
                                (((1,), (1,)), ((), ())), preferred_element_type=jnp.float32)
        for q in range(nr):
            block = total[q * half:(q + 1) * half, :]
            acc[q, 0] += block[:, :LANES]
            acc[q, 1] += block[:, LANES:]

    acc[...] = jnp.zeros_like(acc)

    def wait_for(i):
        pltpu.make_async_remote_copy(
            src_ref=got.at[0], dst_ref=got.at[i], send_sem=gsend.at[i], recv_sem=grecv.at[i],
            device_id={"files": (f + 1) % nf}, device_id_type=MESH).wait_recv()

    def step(t, carry):
        pl.when(t > 0)(lambda: wait_for(t))
        add_points(got[t, 0:blocks, :], got[t, blocks:, :])
        return carry

    lax.fori_loop(0, nf, step, 0)

    backs = []
    for k in tuple(range(2, nr)) + (1,):
        peer = flipped(r, k, nr)
        copy = pltpu.make_async_remote_copy(
            src_ref=acc.at[peer], dst_ref=parts.at[k], send_sem=rsend.at[k], recv_sem=rrecv.at[k],
            device_id={"rep": peer}, device_id_type=MESH)
        copy.start()
        backs.append(copy)
    for copy in sends:
        copy.wait_send()
    for copy in backs:
        copy.wait()
    tot = acc[r]
    for k in range(1, nr):
        tot = tot + parts[k]
    out[...] = tot.reshape(out.shape)


def solution(mesh):
    nf = mesh.shape["files"]
    nr = mesh.shape["rep"]
    owned = TILES // nf
    quarter = TR // nr
    half = owned * quarter // 2

    def per_device(tile_id, pix_row, pix_col, point_value):
        blocks = tile_id.shape[0] // LANES
        shape = (blocks, LANES)
        out = pl.pallas_call(
            functools.partial(kernel, nf, nr, owned, quarter),
            out_shape=jax.ShapeDtypeStruct((2 * half, LANES), jnp.float32),
            in_specs=[pl.BlockSpec(memory_space=pl.ANY)] * 4,
            out_specs=pl.BlockSpec(memory_space=pltpu.VMEM),
            scratch_shapes=[
                pltpu.VMEM(shape, jnp.int32),
                pltpu.VMEM(shape, jnp.int32),
                pltpu.VMEM(shape, jnp.int32),
                pltpu.VMEM(shape, point_value.dtype),
                pltpu.VMEM((nf, 2 * blocks, LANES), jnp.float32),
                pltpu.VMEM((nr, 2, half, LANES), jnp.float32),
                pltpu.VMEM((nr, 2, half, LANES), jnp.float32),
                pltpu.SemaphoreType.DMA((4,)),
                pltpu.SemaphoreType.DMA,
                pltpu.SemaphoreType.DMA((nf,)),
                pltpu.SemaphoreType.DMA((nf,)),
                pltpu.SemaphoreType.DMA((nr,)),
                pltpu.SemaphoreType.DMA((nr,)),
            ],
            compiler_params=pltpu.CompilerParams(collective_id=0, has_side_effects=True, vmem_limit_bytes=12*1024*1024),
        )(*[pltpu.with_memory_space_constraint(x.reshape(shape), pltpu.HBM)
            for x in (tile_id, pix_row, pix_col, point_value)])
        return out.reshape(owned, quarter, LANES)

    both = P(("files", "rep"))
    return jax.shard_map(per_device, mesh=mesh, in_specs=(both,) * 4,
                         out_specs=P("files", "rep", None), check_vma=False)
```

```python
import functools

import jax
import jax.numpy as jnp
from jax import lax
from jax.experimental import pallas as pl
from jax.experimental.pallas import tpu as pltpu
from jax.sharding import PartitionSpec as P

LANES = 128
WIDE = 256
TR = 32
TILES = 128
SLACK = 4
ORDER = (7, 6, 5, 4, 3, 2, 1)
ARRIVE = (1, 2, 3, 6, 4, 7, 5)
MESH = pl.DeviceIdType.MESH
BF16 = jnp.bfloat16


def flipped(index, mask, count):
    out = index
    bit = 1
    while bit < count:
        if mask & bit:
            out = out + (1 - 2 * ((index // bit) % 2)) * bit
        bit *= 2
    return out


def iota(shape, dim):
    return lax.broadcasted_iota(jnp.int32, shape, dim)


def dot(a, b, transposed=False):
    return lax.dot_general(a, b, (((1,), (1 if transposed else 0,)), ((), ())),
                           preferred_element_type=jnp.float32)


def kernel(nf, nr, owned, quarter, cap, tile_ref, row_ref, col_ref, val_ref, out,
           tile_in, row_in, col_in, val_in, packed, got, acc, parts,
           isem, gsend, grecv, rsend, rrecv):
    f = lax.axis_index("files")
    r = lax.axis_index("rep")
    half = owned * quarter // 2
    band = nr * half
    blocks = tile_ref.shape[0]
    width = min(WIDE, cap)
    lines = cap // width
    slots = nf * lines
    rows = cap // LANES

    loads = []
    for i, (src, dst) in enumerate(((tile_ref, tile_in), (row_ref, row_in), (col_ref, col_in), (val_ref, val_in))):
        load = pltpu.make_async_copy(src, dst, isem.at[i])
        load.start()
        loads.append(load)
    barrier = pltpu.get_barrier_semaphore()
    for k in range(1, nf):
        pl.semaphore_signal(barrier, inc=1, device_id={"files": flipped(f, k, nf)}, device_id_type=MESH)
    for k in range(1, nr):
        pl.semaphore_signal(barrier, inc=1, device_id={"rep": flipped(r, k, nr)}, device_id_type=MESH)

    one = jnp.ones((), BF16)
    zero = jnp.zeros((), BF16)
    ids = [(iota((16, LANES), 0) + 16 * i).astype(jnp.float32).astype(BF16) for i in range(WIDE // 16)]
    upto = jnp.where(iota((LANES, 2 * LANES), 0) <= iota((LANES, 2 * LANES), 1), 1.0, 0.0).astype(BF16)
    group = max(1, WIDE // blocks)
    span = group * blocks
    i0 = iota((span, span), 0)
    i1 = iota((span, span), 1)
    above = jnp.where((i1 < i0) & (i1 // blocks == i0 // blocks), 1.0, 0.0).astype(BF16)
    acc[...] = jnp.zeros_like(acc)

    for load in loads:
        load.wait()
    tile = tile_in[...]
    prow = row_in[...]
    owner = tile % nf
    inner = (tile // nf) * quarter + prow % quarter
    place = ((prow // quarter) * half + inner % half).astype(jnp.float32)
    col = ((inner // half) * LANES + col_in[...]).astype(jnp.float32)
    values = val_in[...].astype(jnp.float32)

    rank = jnp.zeros((blocks, LANES), jnp.float32)
    for g in range(0, nf, group):
        mine = [owner == o for o in range(g, g + group)]
        marks = jnp.concatenate([jnp.where(m, 1.0, 0.0) for m in mine], axis=0).astype(BF16)
        run = dot(marks, upto)
        before = dot(above, run[:, LANES:].astype(BF16))
        full = run[:, :LANES] + before - 1.0
        for i, m in enumerate(mine):
            rank = rank + jnp.where(m, full[i * blocks:(i + 1) * blocks, :], 0.0)
    slot = owner.astype(jnp.float32) * cap + rank
    line = jnp.floor(slot * (1.0 / width))
    at = slot - line * width

    def wide(x):
        return jnp.broadcast_to(x, (16, LANES)).astype(BF16)

    def one_hot(x, count, payloads):
        picks = [x == ids[i] for i in range(count // 16)]
        return [jnp.concatenate([jnp.where(m, p, zero) for m in picks], axis=0) for p in payloads]

    lhs = []
    rhs = []
    for j in range(blocks):
        pick = [wide(x[j:j + 1, :]) for x in (line, at, place, col, values)]
        lhs.append(jnp.concatenate(one_hot(pick[0], slots, pick[2:]), axis=0))
        rhs.append(one_hot(pick[1], width, [one])[0])
    moved = dot(jnp.concatenate(lhs, axis=1), jnp.concatenate(rhs, axis=1), True)
    cells = moved[:slots] * WIDE + moved[slots:2 * slots]
    vals = moved[2 * slots:]
    for o in range(nf):
        for h in range(width // LANES):
            piece = (slice(o * lines, (o + 1) * lines), slice(h * LANES, (h + 1) * LANES))
            packed[o, h * lines:(h + 1) * lines, :] = cells[piece]
            packed[o, rows + h * lines:rows + (h + 1) * lines, :] = vals[piece]

    pl.semaphore_wait(barrier, nf + nr - 2)

    sends = []
    for k in ORDER if nf == 8 else range(1, nf):
        to = flipped(f, k, nf)
        copy = pltpu.make_async_remote_copy(
            src_ref=packed.at[to], dst_ref=got.at[k], send_sem=gsend.at[k], recv_sem=grecv.at[k],
            device_id={"files": to}, device_id_type=MESH)
        copy.start()
        sends.append(copy)

    def add_points(cells, values):
        row = jnp.floor(cells * (1.0 / WIDE))
        col = cells - row * WIDE
        lhs = []
        rhs = []
        for j in range(rows):
            row16, col16, val16 = [wide(x[j:j + 1, :]) for x in (row, col, values)]
            lhs.append(one_hot(row16, band, [val16])[0])
            rhs.append(one_hot(col16, WIDE, [one])[0])
        total = dot(jnp.concatenate(lhs, axis=1), jnp.concatenate(rhs, axis=1), True)
        for q in range(nr):
            block = total[q * half:(q + 1) * half, :]
            acc[q, 0] += block[:, :LANES]
            acc[q, 1] += block[:, LANES:]

    add_points(packed[f, 0:rows, :], packed[f, rows:, :])

    def step(t, carry):
        k = t
        if nf == 8:
            k = sum(jnp.where(t == i, mask, 0) for i, mask in enumerate(ARRIVE, 1))
        pltpu.make_async_remote_copy(
            src_ref=packed.at[0], dst_ref=got.at[k], send_sem=gsend.at[k], recv_sem=grecv.at[k],
            device_id={"files": (f + 1) % nf}, device_id_type=MESH).wait_recv()
        add_points(got[k, 0:rows, :], got[k, rows:, :])
        return carry

    lax.fori_loop(1, nf, step, 0)

    backs = []
    for k in tuple(range(2, nr)) + (1,):
        peer = flipped(r, k, nr)
        copy = pltpu.make_async_remote_copy(
            src_ref=acc.at[peer], dst_ref=parts.at[k], send_sem=rsend.at[k], recv_sem=rrecv.at[k],
            device_id={"rep": peer}, device_id_type=MESH)
        copy.start()
        backs.append(copy)
    for copy in sends:
        copy.wait_send()
    for copy in backs:
        copy.wait()
    total = acc[r]
    for k in range(1, nr):
        total = total + parts[k]
    out[...] = total.reshape(out.shape)


def solution(mesh):
    nf = mesh.shape["files"]
    nr = mesh.shape["rep"]
    owned = TILES // nf
    quarter = TR // nr
    half = owned * quarter // 2

    def per_device(tile_id, pix_row, pix_col, point_value):
        points = tile_id.shape[0]
        cap = SLACK * points // nf
        shape = (points // LANES, LANES)
        message = 2 * cap // LANES
        out = pl.pallas_call(
            functools.partial(kernel, nf, nr, owned, quarter, cap),
            out_shape=jax.ShapeDtypeStruct((2 * half, LANES), jnp.float32),
            in_specs=[pl.BlockSpec(memory_space=pl.ANY)] * 4,
            out_specs=pl.BlockSpec(memory_space=pltpu.VMEM),
            scratch_shapes=[
                pltpu.VMEM(shape, jnp.int32),
                pltpu.VMEM(shape, jnp.int32),
                pltpu.VMEM(shape, jnp.int32),
                pltpu.VMEM(shape, point_value.dtype),
                pltpu.VMEM((nf, message, LANES), jnp.float32),
                pltpu.VMEM((nf, message, LANES), jnp.float32),
                pltpu.VMEM((nr, 2, half, LANES), jnp.float32),
                pltpu.VMEM((nr, 2, half, LANES), jnp.float32),
                pltpu.SemaphoreType.DMA((4,)),
                pltpu.SemaphoreType.DMA((nf,)),
                pltpu.SemaphoreType.DMA((nf,)),
                pltpu.SemaphoreType.DMA((nr,)),
                pltpu.SemaphoreType.DMA((nr,)),
            ],
            compiler_params=pltpu.CompilerParams(collective_id=0, has_side_effects=True,
                                                 vmem_limit_bytes=16 * 1024 * 1024),
        )(*[pltpu.with_memory_space_constraint(x.reshape(shape), pltpu.HBM)
            for x in (tile_id, pix_row, pix_col, point_value)])
        return out.reshape(owned, quarter, LANES)

    both = P(("files", "rep"))
    return jax.shard_map(per_device, mesh=mesh, in_specs=(both,) * 4,
                         out_specs=P("files", "rep", None), check_vma=False)
```

```python
import functools

import jax
import jax.numpy as jnp
from jax import lax
from jax.experimental import pallas as pl
from jax.experimental.pallas import tpu as pltpu
from jax.sharding import PartitionSpec as P

LANES = 128
WIDE = 256
TR = 32
TILES = 128
SLACK = 4
MESH = pl.DeviceIdType.MESH
BF16 = jnp.bfloat16


def flipped(index, mask, count):
    out = index
    bit = 1
    while bit < count:
        if mask & bit:
            out = out + (1 - 2 * ((index // bit) % 2)) * bit
        bit *= 2
    return out


def iota(shape, dim):
    return lax.broadcasted_iota(jnp.int32, shape, dim)


def dot(a, b, transposed=False):
    return lax.dot_general(a, b, (((1,), (1 if transposed else 0,)), ((), ())),
                           preferred_element_type=jnp.float32)


def kernel(nf, nr, owned, quarter, cap, tile_ref, row_ref, col_ref, val_ref, out,
           tile_in, row_in, col_in, val_in, packed, got, acc, parts,
           isem, fready, rready, gsend, grecv, rsend, rrecv):
    f = lax.axis_index("files")
    r = lax.axis_index("rep")
    half = owned * quarter // 2
    band = nr * half
    blocks = tile_ref.shape[0]
    width = min(WIDE, cap)
    lines = cap // width
    slots = nf * lines
    rows = cap // LANES

    loads = []
    for i, (src, dst) in enumerate(((tile_ref, tile_in), (row_ref, row_in), (col_ref, col_in), (val_ref, val_in))):
        load = pltpu.make_async_copy(src, dst, isem.at[i])
        load.start()
        loads.append(load)
    barrier = pltpu.get_barrier_semaphore()

    def signal(sem, axis, to):
        pl.semaphore_signal(sem, inc=1, device_id={axis: to}, device_id_type=MESH)

    for i in range(1, nf):
        pl.when(f + i < nf)(functools.partial(signal, barrier, "files", f + i))
    for i in range(1, nr):
        pl.when(r + i < nr)(functools.partial(signal, barrier, "rep", r + i))
    pl.when(f + r > 0)(functools.partial(pl.semaphore_wait, barrier, f + r))
    for i in range(1, nf):
        pl.when(f - i >= 0)(functools.partial(signal, fready.at[f], "files", f - i))
    for i in range(1, nr):
        pl.when(r - i >= 0)(functools.partial(signal, rready.at[r], "rep", r - i))

    one = jnp.ones((), BF16)
    zero = jnp.zeros((), BF16)
    ids = [(iota((16, LANES), 0) + 16 * i).astype(jnp.float32).astype(BF16) for i in range(WIDE // 16)]
    upto = jnp.where(iota((LANES, 2 * LANES), 0) <= iota((LANES, 2 * LANES), 1), 1.0, 0.0).astype(BF16)
    group = max(1, WIDE // blocks)
    span = group * blocks
    i0 = iota((span, span), 0)
    i1 = iota((span, span), 1)
    above = jnp.where((i1 < i0) & (i1 // blocks == i0 // blocks), 1.0, 0.0).astype(BF16)
    acc[...] = jnp.zeros_like(acc)

    for load in loads:
        load.wait()
    tile = tile_in[...]
    prow = row_in[...]
    owner = tile % nf
    inner = (tile // nf) * quarter + prow % quarter
    place = ((prow // quarter) * half + inner % half).astype(jnp.float32)
    col = ((inner // half) * LANES + col_in[...]).astype(jnp.float32)
    values = val_in[...].astype(jnp.float32)

    rank = jnp.zeros((blocks, LANES), jnp.float32)
    for g in range(0, nf, group):
        mine = [owner == o for o in range(g, g + group)]
        marks = jnp.concatenate([jnp.where(m, 1.0, 0.0) for m in mine], axis=0).astype(BF16)
        run = dot(marks, upto)
        before = dot(above, run[:, LANES:].astype(BF16))
        full = run[:, :LANES] + before - 1.0
        for i, m in enumerate(mine):
            rank = rank + jnp.where(m, full[i * blocks:(i + 1) * blocks, :], 0.0)
    slot = owner.astype(jnp.float32) * cap + rank
    line = jnp.floor(slot * (1.0 / width))
    at = slot - line * width

    def wide(x):
        return jnp.broadcast_to(x, (16, LANES)).astype(BF16)

    def one_hot(x, count, payloads):
        picks = [x == ids[i] for i in range(count // 16)]
        return [jnp.concatenate([jnp.where(m, p, zero) for m in picks], axis=0) for p in payloads]

    lhs = []
    rhs = []
    for j in range(blocks):
        pick = [wide(x[j:j + 1, :]) for x in (line, at, place, col, values)]
        lhs.append(jnp.concatenate(one_hot(pick[0], slots, pick[2:]), axis=0))
        rhs.append(one_hot(pick[1], width, [one])[0])
    moved = dot(jnp.concatenate(lhs, axis=1), jnp.concatenate(rhs, axis=1), True)
    cells = moved[:slots] * WIDE + moved[slots:2 * slots]
    vals = moved[2 * slots:]
    for o in range(nf):
        for h in range(width // LANES):
            piece = (slice(o * lines, (o + 1) * lines), slice(h * LANES, (h + 1) * LANES))
            packed[o, h * lines:(h + 1) * lines, :] = cells[piece]
            packed[o, rows + h * lines:rows + (h + 1) * lines, :] = vals[piece]

    def send(to):
        return pltpu.make_async_remote_copy(
            src_ref=packed.at[to], dst_ref=got.at[f], send_sem=gsend.at[to], recv_sem=grecv.at[f],
            device_id={"files": to}, device_id_type=MESH)

    def receive(source):
        return pltpu.make_async_remote_copy(
            src_ref=packed.at[f], dst_ref=got.at[source], send_sem=gsend.at[f], recv_sem=grecv.at[source],
            device_id={"files": source}, device_id_type=MESH)

    for to in range(nf - 1):
        pl.when(to < f)(lambda to=to: send(to).start())

    def add_points(chunks):
        lhs = []
        rhs = []
        for chunk in chunks:
            cells = chunk[0:rows, :]
            row = jnp.floor(cells * (1.0 / WIDE))
            col = cells - row * WIDE
            for j in range(rows):
                row16, col16, val16 = [wide(x[j:j + 1, :]) for x in (row, col, chunk[rows:, :])]
                lhs.append(one_hot(row16, band, [val16])[0])
                rhs.append(one_hot(col16, WIDE, [one])[0])
        total = dot(jnp.concatenate(lhs, axis=1), jnp.concatenate(rhs, axis=1), True)
        for q in range(nr):
            block = total[q * half:(q + 1) * half, :]
            acc[q, 0] += block[:, :LANES]
            acc[q, 1] += block[:, LANES:]

    got[f] = packed[f]

    for i in range(1, nf):
        @pl.when(f + i < nf)
        def _():
            pl.semaphore_wait(fready.at[f + i], 1)
            send(f + i).start()

    def arrived(k):
        source = f
        bit = 1
        while bit < nf:
            source = source + (1 - 2 * ((f // bit) % 2)) * bit * ((k // bit) % 2)
            bit *= 2
        pl.when(k > 0)(lambda: receive(source).wait_recv())
        return source

    def step(t, carry):
        k = 2 * t
        if nf == 8:
            k = k + jnp.where(((f // 2) % 3 > 0) & (t >= 2), 2 - 4 * (t % 2), 0)
        pair = [arrived(k), arrived(k + 1)]
        add_points([got[source] for source in pair])
        return carry

    lax.fori_loop(0, nf // 2, step, 0)

    for i in range(1, nr):
        @pl.when(r + i < nr)
        def _():
            pl.semaphore_wait(rready.at[r + i], 1)
    backs = []
    for k in tuple(range(2, nr)) + (1,):
        peer = flipped(r, k, nr)
        copy = pltpu.make_async_remote_copy(
            src_ref=acc.at[peer], dst_ref=parts.at[k], send_sem=rsend.at[k], recv_sem=rrecv.at[k],
            device_id={"rep": peer}, device_id_type=MESH)
        copy.start()
        backs.append(copy)
    for to in range(nf):
        pl.when(to != f)(lambda to=to: send(to).wait_send())
    for copy in backs:
        copy.wait()
    total = acc[r]
    for k in range(1, nr):
        total = total + parts[k]
    out[...] = total.reshape(out.shape)


def solution(mesh):
    nf = mesh.shape["files"]
    nr = mesh.shape["rep"]
    owned = TILES // nf
    quarter = TR // nr
    half = owned * quarter // 2

    def per_device(tile_id, pix_row, pix_col, point_value):
        points = tile_id.shape[0]
        cap = SLACK * points // nf
        shape = (points // LANES, LANES)
        message = 2 * cap // LANES
        out = pl.pallas_call(
            functools.partial(kernel, nf, nr, owned, quarter, cap),
            out_shape=jax.ShapeDtypeStruct((2 * half, LANES), jnp.float32),
            in_specs=[pl.BlockSpec(memory_space=pl.ANY)] * 4,
            out_specs=pl.BlockSpec(memory_space=pltpu.VMEM),
            scratch_shapes=[
                pltpu.VMEM(shape, jnp.int32),
                pltpu.VMEM(shape, jnp.int32),
                pltpu.VMEM(shape, jnp.int32),
                pltpu.VMEM(shape, point_value.dtype),
                pltpu.VMEM((nf, message, LANES), jnp.float32),
                pltpu.VMEM((nf, message, LANES), jnp.float32),
                pltpu.VMEM((nr, 2, half, LANES), jnp.float32),
                pltpu.VMEM((nr, 2, half, LANES), jnp.float32),
                pltpu.SemaphoreType.DMA((4,)),
                pltpu.SemaphoreType.REGULAR((nf,)),
                pltpu.SemaphoreType.REGULAR((nr,)),
                pltpu.SemaphoreType.DMA((nf,)),
                pltpu.SemaphoreType.DMA((nf,)),
                pltpu.SemaphoreType.DMA((nr,)),
                pltpu.SemaphoreType.DMA((nr,)),
            ],
            compiler_params=pltpu.CompilerParams(collective_id=0, has_side_effects=True,
                                                 vmem_limit_bytes=16 * 1024 * 1024),
        )(*[pltpu.with_memory_space_constraint(x.reshape(shape), pltpu.HBM)
            for x in (tile_id, pix_row, pix_col, point_value)])
        return out.reshape(owned, quarter, LANES)

    both = P(("files", "rep"))
    return jax.shard_map(per_device, mesh=mesh, in_specs=(both,) * 4,
                         out_specs=P("files", "rep", None), check_vma=False)
```

```python
import functools

import jax
import jax.numpy as jnp
from jax import lax
from jax.experimental import pallas as pl
from jax.experimental.pallas import tpu as pltpu
from jax.sharding import PartitionSpec as P

LANES = 128
WIDE = 256
TR = 32
TILES = 128
SLACK = 4
PAIRS = ((0, 2, 4, 6), (0, 2, 6, 4), (0, 6, 2, 4), (0, 2, 4, 6))
MESH = pl.DeviceIdType.MESH
BF16 = jnp.bfloat16


def flipped(index, mask, count):
    out = index
    bit = 1
    while bit < count:
        if mask & bit:
            out = out + (1 - 2 * ((index // bit) % 2)) * bit
        bit *= 2
    return out


def iota(shape, dim):
    return lax.broadcasted_iota(jnp.int32, shape, dim)


def dot(a, b, transposed=False):
    return lax.dot_general(a, b, (((1,), (1 if transposed else 0,)), ((), ())),
                           preferred_element_type=jnp.float32)


def kernel(nf, nr, owned, quarter, cap, tile_ref, row_ref, col_ref, val_ref, parts,
           tile_in, row_in, col_in, val_in, packed, got, acc,
           fready, rready, gsend, grecv, rsend, rrecv):
    f = lax.axis_index("files")
    r = lax.axis_index("rep")
    half = owned * quarter // 2
    band = nr * half
    blocks = tile_ref.shape[0]
    width = min(WIDE, cap)
    lines = cap // width
    slots = nf * lines
    rows = cap // LANES

    loads = []
    for i, (src, dst) in enumerate(((tile_ref, tile_in), (row_ref, row_in), (col_ref, col_in), (val_ref, val_in))):
        load = pltpu.make_async_copy(src, dst, rsend.at[i])
        load.start()
        loads.append(load)
    barrier = pltpu.get_barrier_semaphore()

    def signal(sem, axis, to):
        pl.semaphore_signal(sem, inc=1, device_id={axis: to}, device_id_type=MESH)

    for i in range(1, nf):
        pl.when(f + i < nf)(functools.partial(signal, barrier, "files", f + i))
    for i in range(1, nr):
        pl.when(r + i < nr)(functools.partial(signal, barrier, "rep", r + i))
    def enter():
        pl.when(f + r > 0)(functools.partial(pl.semaphore_wait, barrier, f + r))
        for i in range(1, nf):
            pl.when(f - i >= 0)(functools.partial(signal, fready.at[f // 2], "files", f - i))
        for i in range(1, nr):
            pl.when(r - i >= 0)(functools.partial(signal, rready, "rep", r - i))

    pl.when(f >= nf - 2)(enter)

    one = jnp.ones((), BF16)
    zero = jnp.zeros((), BF16)
    ids = [(iota((16, LANES), 0) + 16 * i).astype(jnp.float32).astype(BF16) for i in range(WIDE // 16)]
    upto = jnp.where(iota((LANES, 2 * LANES), 0) <= iota((LANES, 2 * LANES), 1), 1.0, 0.0).astype(BF16)
    group = max(1, WIDE // blocks)
    span = group * blocks
    i0 = iota((span, span), 0)
    i1 = iota((span, span), 1)
    above = jnp.where((i1 < i0) & (i1 // blocks == i0 // blocks), 1.0, 0.0).astype(BF16)
    acc[...] = jnp.zeros_like(acc)

    for load in loads:
        load.wait()
    tile = tile_in[...]
    prow = row_in[...]
    owner = tile % nf
    inner = (tile // nf) * quarter + prow % quarter
    place = ((prow // quarter) * half + inner % half).astype(jnp.float32)
    col = ((inner // half) * LANES + col_in[...]).astype(jnp.float32)
    values = val_in[...].astype(jnp.float32)

    rank = jnp.zeros((blocks, LANES), jnp.float32)
    for g in range(0, nf, group):
        mine = [owner == o for o in range(g, g + group)]
        marks = jnp.concatenate([jnp.where(m, 1.0, 0.0) for m in mine], axis=0).astype(BF16)
        run = dot(marks, upto)
        before = dot(above, run[:, LANES:].astype(BF16))
        full = run[:, :LANES] + before - 1.0
        for i, m in enumerate(mine):
            rank = rank + jnp.where(m, full[i * blocks:(i + 1) * blocks, :], 0.0)
    pl.when(f < nf - 2)(enter)
    slot = owner.astype(jnp.float32) * cap + rank
    line = jnp.floor(slot * (1.0 / width))
    at = slot - line * width

    def wide(x):
        return jnp.broadcast_to(x, (16, LANES)).astype(BF16)

    def one_hot(x, count, payloads):
        picks = [x == ids[i] for i in range(count // 16)]
        return [jnp.concatenate([jnp.where(m, p, zero) for m in picks], axis=0) for p in payloads]

    lhs = []
    rhs = []
    for j in range(blocks):
        pick = [wide(x[j:j + 1, :]) for x in (line, at, place, col, values)]
        lhs.append(jnp.concatenate(one_hot(pick[0], slots, pick[2:]), axis=0))
        rhs.append(one_hot(pick[1], width, [one])[0])
    moved = dot(jnp.concatenate(lhs, axis=1), jnp.concatenate(rhs, axis=1), True)
    cells = moved[:slots] * WIDE + moved[slots:2 * slots]
    vals = moved[2 * slots:]
    for o in range(nf):
        for h in range(width // LANES):
            piece = (slice(o * lines, (o + 1) * lines), slice(h * LANES, (h + 1) * LANES))
            packed[o, h * lines:(h + 1) * lines, :] = cells[piece]
            packed[o, rows + h * lines:rows + (h + 1) * lines, :] = vals[piece]

    def send(to):
        return pltpu.make_async_remote_copy(
            src_ref=packed.at[to], dst_ref=got.at[f], send_sem=gsend, recv_sem=grecv.at[f],
            device_id={"files": to}, device_id_type=MESH)

    def receive(source):
        return pltpu.make_async_remote_copy(
            src_ref=packed.at[f], dst_ref=got.at[source], send_sem=gsend, recv_sem=grecv.at[source],
            device_id={"files": source}, device_id_type=MESH)

    for to in range(nf - 1):
        pl.when(to < f)(lambda to=to: send(to).start())

    def add_points(chunks):
        lhs = []
        rhs = []
        for chunk in chunks:
            cells = chunk[0:rows, :]
            row = jnp.floor(cells * (1.0 / WIDE))
            col = cells - row * WIDE
            for j in range(rows):
                row16, col16, val16 = [wide(x[j:j + 1, :]) for x in (row, col, chunk[rows:, :])]
                lhs.append(one_hot(row16, band, [val16])[0])
                rhs.append(one_hot(col16, WIDE, [one])[0])
        total = dot(jnp.concatenate(lhs, axis=1), jnp.concatenate(rhs, axis=1), True)
        for q in range(nr):
            block = total[q * half:(q + 1) * half, :]
            acc[q, 0] += block[:, :LANES]
            acc[q, 1] += block[:, LANES:]

    got[f] = packed[f]

    @pl.when(f % 2 == 0)
    def _():
        pl.semaphore_wait(fready.at[f // 2], 1)
        send(f + 1).start()

    for i in range(1, nf // 2):
        @pl.when(f // 2 + i < nf // 2)
        def _():
            pl.semaphore_wait(fready.at[f // 2 + i], 2)
            send((f // 2 + i) * 2).start()
            send((f // 2 + i) * 2 + 1).start()

    def arrived(k):
        source = f
        bit = 1
        while bit < nf:
            source = source + (1 - 2 * ((f // bit) % 2)) * bit * ((k // bit) % 2)
            bit *= 2
        pl.when(k > 0)(lambda: receive(source).wait_recv())
        return source

    def step(t, carry):
        k = 2 * t
        if nf == 8:
            k = sum(jnp.where((f // 2 == z) & (t == i), first, 0)
                    for z, order in enumerate(PAIRS) for i, first in enumerate(order))
        pair = [arrived(k), arrived(k + 1)]
        add_points([got[source] for source in pair])
        return carry

    lax.fori_loop(0, nf // 2, step, 0)

    pl.when(r < nr - 1)(functools.partial(pl.semaphore_wait, rready, nr - 1 - r))
    backs = []
    for k in tuple(range(2, nr)) + (1,):
        peer = flipped(r, k, nr)
        copy = pltpu.make_async_remote_copy(
            src_ref=acc.at[peer], dst_ref=parts.at[k], send_sem=rsend.at[k], recv_sem=rrecv.at[k],
            device_id={"rep": peer}, device_id_type=MESH)
        copy.start()
        backs.append(copy)
    parts[0] = acc[r]
    pltpu.make_async_remote_copy(
        src_ref=packed.at[pl.ds(0, nf - 1)], dst_ref=got.at[pl.ds(0, nf - 1)], send_sem=gsend, recv_sem=grecv.at[0],
        device_id={"files": f}, device_id_type=MESH).wait_send()
    for copy in backs:
        copy.wait()


def solution(mesh):
    nf = mesh.shape["files"]
    nr = mesh.shape["rep"]
    owned = TILES // nf
    quarter = TR // nr
    half = owned * quarter // 2

    def per_device(tile_id, pix_row, pix_col, point_value):
        points = tile_id.shape[0]
        cap = SLACK * points // nf
        shape = (points // LANES, LANES)
        message = 2 * cap // LANES
        out = pl.pallas_call(
            functools.partial(kernel, nf, nr, owned, quarter, cap),
            out_shape=jax.ShapeDtypeStruct((nr, 2, half, LANES), jnp.float32),
            in_specs=[pl.BlockSpec(memory_space=pl.ANY)] * 4,
            out_specs=pl.BlockSpec(memory_space=pltpu.VMEM),
            scratch_shapes=[
                pltpu.VMEM(shape, jnp.int32),
                pltpu.VMEM(shape, jnp.int32),
                pltpu.VMEM(shape, jnp.int32),
                pltpu.VMEM(shape, point_value.dtype),
                pltpu.VMEM((nf, message, LANES), jnp.float32),
                pltpu.VMEM((nf, message, LANES), jnp.float32),
                pltpu.VMEM((nr, 2, half, LANES), jnp.float32),
                pltpu.SemaphoreType.REGULAR((nf // 2,)),
                pltpu.SemaphoreType.REGULAR,
                pltpu.SemaphoreType.DMA,
                pltpu.SemaphoreType.DMA((nf,)),
                pltpu.SemaphoreType.DMA((max(nr, 4),)),
                pltpu.SemaphoreType.DMA((nr,)),
            ],
            compiler_params=pltpu.CompilerParams(collective_id=0, has_side_effects=True,
                                                 vmem_limit_bytes=16 * 1024 * 1024),
        )(*[pltpu.with_memory_space_constraint(x.reshape(shape), pltpu.HBM)
            for x in (tile_id, pix_row, pix_col, point_value)])
        return jnp.sum(out, axis=0).reshape(owned, quarter, LANES)

    both = P(("files", "rep"))
    return jax.shard_map(per_device, mesh=mesh, in_specs=(both,) * 4,
                         out_specs=P("files", "rep", None), check_vma=False)
```

```python
import functools

import jax
import jax.numpy as jnp
from jax import lax
from jax.experimental import pallas as pl
from jax.experimental.pallas import tpu as pltpu
from jax.sharding import PartitionSpec as P

LANES = 128
WIDE = 256
TR = 32
TILES = 128
SLACK = 4
CROSS_AFTER = 5
PAIRS = ((0, 2, 4, 6), (0, 2, 6, 4), (0, 6, 2, 4), (0, 2, 4, 6))
MESH = pl.DeviceIdType.MESH
BF16 = jnp.bfloat16


def flipped(index, mask, count):
    out = index
    bit = 1
    while bit < count:
        if mask & bit:
            out = out + (1 - 2 * ((index // bit) % 2)) * bit
        bit *= 2
    return out


def iota(shape, dim):
    return lax.broadcasted_iota(jnp.int32, shape, dim)


def dot(a, b, transposed=False):
    return lax.dot_general(a, b, (((1,), (1 if transposed else 0,)), ((), ())),
                           preferred_element_type=jnp.float32)


def kernel(nf, nr, owned, quarter, cap, tile_ref, row_ref, col_ref, val_ref, parts,
           tile_in, row_in, col_in, val_in, packed, got, acc, side,
           fready, rready, gsend, grecv, rsend, rrecv):
    f = lax.axis_index("files")
    r = lax.axis_index("rep")
    half = owned * quarter // 2
    band = nr * half
    direct = nf == 8 and nr == 4
    top = nf - 2
    blocks = tile_ref.shape[0]
    width = min(WIDE, cap)
    lines = cap // width
    slots = nf * lines
    rows = cap // LANES

    loads = []
    for i, (src, dst) in enumerate(((tile_ref, tile_in), (row_ref, row_in), (col_ref, col_in), (val_ref, val_in))):
        load = pltpu.make_async_copy(src, dst, rsend.at[i])
        load.start()
        loads.append(load)
    barrier = pltpu.get_barrier_semaphore()

    def signal(sem, axis, to):
        pl.semaphore_signal(sem, inc=1, device_id={axis: to}, device_id_type=MESH)

    for i in range(1, nf):
        pl.when(f + i < nf)(functools.partial(signal, barrier, "files", f + i))
    for i in range(1, nr):
        pl.when(r + i < nr)(functools.partial(signal, barrier, "rep", r + i))
    if direct:
        @pl.when(f < 2)
        def _():
            for to in (top, top + 1):
                pl.semaphore_signal(barrier, inc=1, device_id={"files": to, "rep": flipped(r, 2, nr)},
                                    device_id_type=MESH)
    entered = f + r + (jnp.where(f >= top, 2, 0) if direct else 0)

    def enter():
        pl.when(entered > 0)(functools.partial(pl.semaphore_wait, barrier, entered))
        for i in range(1, nf):
            pl.when(f - i >= 0)(functools.partial(signal, fready.at[f // 2], "files", f - i))
        for i in range(1, nr):
            pl.when(r - i >= 0)(functools.partial(signal, rready, "rep", r - i))

    pl.when(f >= nf - 2)(enter)

    one = jnp.ones((), BF16)
    zero = jnp.zeros((), BF16)
    ids = [(iota((16, LANES), 0) + 16 * i).astype(jnp.float32).astype(BF16) for i in range(WIDE // 16)]
    upto = jnp.where(iota((LANES, 2 * LANES), 0) <= iota((LANES, 2 * LANES), 1), 1.0, 0.0).astype(BF16)
    group = max(1, WIDE // blocks)
    span = group * blocks
    i0 = iota((span, span), 0)
    i1 = iota((span, span), 1)
    above = jnp.where((i1 < i0) & (i1 // blocks == i0 // blocks), 1.0, 0.0).astype(BF16)
    acc[...] = jnp.zeros_like(acc)

    for load in loads:
        load.wait()
    tile = tile_in[...]
    prow = row_in[...]
    owner = tile % nf
    inner = (tile // nf) * quarter + prow % quarter
    place = ((prow // quarter) * half + inner % half).astype(jnp.float32)
    col = ((inner // half) * LANES + col_in[...]).astype(jnp.float32)
    values = val_in[...].astype(jnp.float32)

    rank = jnp.zeros((blocks, LANES), jnp.float32)
    for g in range(0, nf, group):
        mine = [owner == o for o in range(g, g + group)]
        marks = jnp.concatenate([jnp.where(m, 1.0, 0.0) for m in mine], axis=0).astype(BF16)
        run = dot(marks, upto)
        before = dot(above, run[:, LANES:].astype(BF16))
        full = run[:, :LANES] + before - 1.0
        for i, m in enumerate(mine):
            rank = rank + jnp.where(m, full[i * blocks:(i + 1) * blocks, :], 0.0)
    pl.when(f < nf - 2)(enter)
    slot = owner.astype(jnp.float32) * cap + rank
    line = jnp.floor(slot * (1.0 / width))
    at = slot - line * width

    def wide(x):
        return jnp.broadcast_to(x, (16, LANES)).astype(BF16)

    def one_hot(x, count, payloads):
        picks = [x == ids[i] for i in range(count // 16)]
        return [jnp.concatenate([jnp.where(m, p, zero) for m in picks], axis=0) for p in payloads]

    lhs = []
    rhs = []
    for j in range(blocks):
        pick = [wide(x[j:j + 1, :]) for x in (line, at, place, col, values)]
        lhs.append(jnp.concatenate(one_hot(pick[0], slots, pick[2:]), axis=0))
        rhs.append(one_hot(pick[1], width, [one])[0])
    moved = dot(jnp.concatenate(lhs, axis=1), jnp.concatenate(rhs, axis=1), True)
    cells = moved[:slots] * WIDE + moved[slots:2 * slots]
    vals = moved[2 * slots:]
    for o in range(nf):
        for h in range(width // LANES):
            piece = (slice(o * lines, (o + 1) * lines), slice(h * LANES, (h + 1) * LANES))
            packed[o, h * lines:(h + 1) * lines, :] = cells[piece]
            packed[o, rows + h * lines:rows + (h + 1) * lines, :] = vals[piece]

    def send(to):
        return pltpu.make_async_remote_copy(
            src_ref=packed.at[to], dst_ref=got.at[f], send_sem=gsend, recv_sem=grecv.at[f],
            device_id={"files": to}, device_id_type=MESH)

    def receive(source):
        return pltpu.make_async_remote_copy(
            src_ref=packed.at[f], dst_ref=got.at[source], send_sem=gsend, recv_sem=grecv.at[source],
            device_id={"files": source}, device_id_type=MESH)

    def cross(to):
        return pltpu.make_async_remote_copy(
            src_ref=packed.at[to], dst_ref=got.at[nf + f % 2], send_sem=gsend, recv_sem=grecv.at[nf + f % 2],
            device_id={"files": to, "rep": flipped(r, 2, nr)}, device_id_type=MESH)

    for to in range(nf - 1):
        pl.when(to < f)(lambda to=to: send(to).start())
        if direct and to == CROSS_AFTER:
            @pl.when(f >= top)
            def _():
                cross(0).start()
                cross(1).start()

    def add_points(chunks, base, count):
        lhs = []
        rhs = []
        for chunk in chunks:
            cells = chunk[0:rows, :]
            row = jnp.floor(cells * (1.0 / WIDE))
            col = cells - row * WIDE
            if count < nr:
                row = row - (base * half).astype(jnp.float32)
            for j in range(rows):
                row16, col16, val16 = [wide(x[j:j + 1, :]) for x in (row, col, chunk[rows:, :])]
                lhs.append(one_hot(row16, count * half, [val16])[0])
                rhs.append(one_hot(col16, WIDE, [one])[0])
        total = dot(jnp.concatenate(lhs, axis=1), jnp.concatenate(rhs, axis=1), True)
        for q in range(count):
            block = total[q * half:(q + 1) * half, :]
            acc[base + q, 0] += block[:, :LANES]
            acc[base + q, 1] += block[:, LANES:]

    got[f] = packed[f]

    @pl.when(f % 2 == 0)
    def _():
        pl.semaphore_wait(fready.at[f // 2], 1)
        send(f + 1).start()

    for i in range(1, nf // 2):
        @pl.when(f // 2 + i < nf // 2)
        def _():
            pl.semaphore_wait(fready.at[f // 2 + i], 2)
            send((f // 2 + i) * 2).start()
            send((f // 2 + i) * 2 + 1).start()

    def arrived(k):
        source = f
        bit = 1
        while bit < nf:
            source = source + (1 - 2 * ((f // bit) % 2)) * bit * ((k // bit) % 2)
            bit *= 2
        pl.when(k > 0)(lambda: receive(source).wait_recv())
        return source

    def step(t, carry):
        k = 2 * t
        if nf == 8:
            k = sum(jnp.where((f // 2 == z) & (t == i), first, 0)
                    for z, order in enumerate(PAIRS) for i, first in enumerate(order))
        pair = [arrived(k), arrived(k + 1)]
        add_points([got[source] for source in pair], 0, nr)
        return carry

    lax.fori_loop(0, nf // 2 - (jnp.where(f < 2, 1, 0) if direct else 0), step, 0)

    pl.when(r < nr - 1)(functools.partial(pl.semaphore_wait, rready, nr - 1 - r))
    even = r % 2 == 0
    odd = r % 2 == 1
    sibling = flipped(r, 1, nr)
    firsts = range(2, nr, 2)
    seconds = range(3, nr, 2)

    def pass_on(src, dst, i, to):
        return pltpu.make_async_remote_copy(
            src_ref=src, dst_ref=dst, send_sem=rsend.at[i], recv_sem=rrecv.at[i],
            device_id={"rep": to}, device_id_type=MESH)

    def across(k):
        return pass_on(acc.at[flipped(r, k, nr)], parts.at[k], k, flipped(r, k, nr))

    def aside(k):
        return pass_on(acc.at[flipped(r, k + 1, nr)], side.at[k // 2 - 1], nr + k // 2 - 1, sibling)

    def joined(k):
        return pass_on(side.at[k // 2 - 1], parts.at[k], k, flipped(r, k, nr))

    def join():
        @pl.when(odd)
        def _():
            for k in firsts:
                aside(k).wait_recv()
                side[k // 2 - 1] += acc[flipped(r, k, nr)]
                joined(k).start()

    @pl.when(even)
    def _():
        for k in firsts:
            across(k).start()
            aside(k).start()

    @pl.when(odd)
    def _():
        for k in seconds:
            across(k).start()
            parts[k] = jnp.zeros((2, half, LANES), jnp.float32)

    if direct:
        def late(t, carry):
            pl.when(t == 1)(join)
            pair = [top + 2 * t, top + 2 * t + 1]
            for source in pair:
                pltpu.make_async_remote_copy(
                    src_ref=packed.at[f], dst_ref=got.at[source], send_sem=gsend, recv_sem=grecv.at[source],
                    device_id={"files": (f + 1) % nf}, device_id_type=MESH).wait_recv()
            add_points([got[source] for source in pair], (r // 2) * 2, 2)
            return carry

        lax.fori_loop(0, jnp.where(f < 2, 2, 0), late, 0)
        pl.when(f >= 2)(join)
    else:
        join()
    across(1).start()
    parts[0] = acc[r]
    pltpu.make_async_remote_copy(
        src_ref=packed.at[pl.ds(0, nf - 1)], dst_ref=got.at[pl.ds(0, nf - 1)], send_sem=gsend, recv_sem=grecv.at[0],
        device_id={"files": f}, device_id_type=MESH).wait_send()
    if direct:
        @pl.when(f >= top)
        def _():
            pltpu.make_async_remote_copy(
                src_ref=packed.at[pl.ds(0, 2)], dst_ref=got.at[pl.ds(0, 2)], send_sem=gsend,
                recv_sem=grecv.at[0], device_id={"files": f}, device_id_type=MESH).wait_send()
    across(1).wait()
    for k in firsts:
        across(k).wait()

    @pl.when(even)
    def _():
        for k in firsts:
            aside(k).wait_send()
        for k in seconds:
            across(k).wait_recv()

    @pl.when(odd)
    def _():
        for k in seconds:
            across(k).wait_send()


def solution(mesh):
    nf = mesh.shape["files"]
    nr = mesh.shape["rep"]
    owned = TILES // nf
    quarter = TR // nr
    half = owned * quarter // 2

    def per_device(tile_id, pix_row, pix_col, point_value):
        points = tile_id.shape[0]
        cap = SLACK * points // nf
        shape = (points // LANES, LANES)
        message = 2 * cap // LANES
        out = pl.pallas_call(
            functools.partial(kernel, nf, nr, owned, quarter, cap),
            out_shape=jax.ShapeDtypeStruct((nr, 2, half, LANES), jnp.float32),
            in_specs=[pl.BlockSpec(memory_space=pl.ANY)] * 4,
            out_specs=pl.BlockSpec(memory_space=pltpu.VMEM),
            scratch_shapes=[
                pltpu.VMEM(shape, jnp.int32),
                pltpu.VMEM(shape, jnp.int32),
                pltpu.VMEM(shape, jnp.int32),
                pltpu.VMEM(shape, point_value.dtype),
                pltpu.VMEM((nf, message, LANES), jnp.float32),
                pltpu.VMEM((nf + 2, message, LANES), jnp.float32),
                pltpu.VMEM((nr, 2, half, LANES), jnp.float32),
                pltpu.VMEM((nr // 2 - 1, 2, half, LANES), jnp.float32),
                pltpu.SemaphoreType.REGULAR((nf // 2,)),
                pltpu.SemaphoreType.REGULAR,
                pltpu.SemaphoreType.DMA,
                pltpu.SemaphoreType.DMA((nf + 2,)),
                pltpu.SemaphoreType.DMA((nr + nr // 2 - 1,)),
                pltpu.SemaphoreType.DMA((nr + nr // 2 - 1,)),
            ],
            compiler_params=pltpu.CompilerParams(collective_id=0, has_side_effects=True,
                                                 vmem_limit_bytes=16 * 1024 * 1024),
        )(*[pltpu.with_memory_space_constraint(x.reshape(shape), pltpu.HBM)
            for x in (tile_id, pix_row, pix_col, point_value)])
        return jnp.sum(out, axis=0).reshape(owned, quarter, LANES)

    both = P(("files", "rep"))
    return jax.shard_map(per_device, mesh=mesh, in_specs=(both,) * 4,
                         out_specs=P("files", "rep", None), check_vma=False)
```

```python
import functools

import jax
import jax.numpy as jnp
from jax import lax
from jax.experimental import pallas as pl
from jax.experimental.pallas import tpu as pltpu
from jax.sharding import PartitionSpec as P

LANES = 128
WIDE = 256
TR = 32
TILES = 128
SLACK = 4
CROSS_AFTER = (1, 5)
PAIRS = ((0, 2, 4, 6), (0, 2, 6, 4), (0, 6, 2, 4), (0, 2, 4, 6))
MESH = pl.DeviceIdType.MESH
BF16 = jnp.bfloat16


def flipped(index, mask, count):
    out = index
    bit = 1
    while bit < count:
        if mask & bit:
            out = out + (1 - 2 * ((index // bit) % 2)) * bit
        bit *= 2
    return out


def iota(shape, dim):
    return lax.broadcasted_iota(jnp.int32, shape, dim)


def dot(a, b, transposed=False):
    return lax.dot_general(a, b, (((1,), (1 if transposed else 0,)), ((), ())),
                           preferred_element_type=jnp.float32)


def kernel(nf, nr, owned, quarter, cap, tile_ref, row_ref, col_ref, val_ref, parts,
           tile_in, row_in, col_in, val_in, packed, got, acc, side,
           fready, rready, gsend, grecv, rsend, rrecv):
    f = lax.axis_index("files")
    r = lax.axis_index("rep")
    half = owned * quarter // 2
    band = nr * half
    direct = nf == 8 and nr == 4
    top = nf - 2
    blocks = tile_ref.shape[0]
    width = min(WIDE, cap)
    lines = cap // width
    slots = nf * lines
    rows = cap // LANES

    loads = []
    for i, (src, dst) in enumerate(((tile_ref, tile_in), (row_ref, row_in), (col_ref, col_in), (val_ref, val_in))):
        load = pltpu.make_async_copy(src, dst, rsend.at[i])
        load.start()
        loads.append(load)
    barrier = pltpu.get_barrier_semaphore()

    def signal(sem, axis, to):
        pl.semaphore_signal(sem, inc=1, device_id={axis: to}, device_id_type=MESH)

    for i in range(1, nf):
        pl.when(f + i < nf)(functools.partial(signal, barrier, "files", f + i))
    for i in range(1, nr):
        pl.when(r + i < nr)(functools.partial(signal, barrier, "rep", r + i))
    if direct:
        @pl.when(f < 2)
        def _():
            for to in (top, top + 1):
                pl.semaphore_signal(barrier, inc=1, device_id={"files": to, "rep": flipped(r, 2, nr)},
                                    device_id_type=MESH)
    entered = f + r + (jnp.where(f >= top, 2, 0) if direct else 0)

    def enter():
        pl.when(entered > 0)(functools.partial(pl.semaphore_wait, barrier, entered))
        for i in range(1, nf):
            pl.when(f - i >= 0)(functools.partial(signal, fready.at[f // 2], "files", f - i))
        for i in range(1, nr):
            pl.when(r - i >= 0)(functools.partial(signal, rready, "rep", r - i))

    pl.when(f >= nf - 2)(enter)

    one = jnp.ones((), BF16)
    zero = jnp.zeros((), BF16)
    ids = [(iota((16, LANES), 0) + 16 * i).astype(jnp.float32).astype(BF16) for i in range(WIDE // 16)]
    upto = jnp.where(iota((LANES, 2 * LANES), 0) <= iota((LANES, 2 * LANES), 1), 1.0, 0.0).astype(BF16)
    group = max(1, WIDE // blocks)
    span = group * blocks
    i0 = iota((span, span), 0)
    i1 = iota((span, span), 1)
    above = jnp.where((i1 < i0) & (i1 // blocks == i0 // blocks), 1.0, 0.0).astype(BF16)
    acc[...] = jnp.zeros_like(acc)

    for load in loads:
        load.wait()
    tile = tile_in[...]
    prow = row_in[...]
    owner = tile % nf
    inner = (tile // nf) * quarter + prow % quarter
    place = ((prow // quarter) * half + inner % half).astype(jnp.float32)
    col = ((inner // half) * LANES + col_in[...]).astype(jnp.float32)
    values = val_in[...].astype(jnp.float32)

    rank = jnp.zeros((blocks, LANES), jnp.float32)
    for g in range(0, nf, group):
        mine = [owner == o for o in range(g, g + group)]
        marks = jnp.concatenate([jnp.where(m, 1.0, 0.0) for m in mine], axis=0).astype(BF16)
        run = dot(marks, upto)
        before = dot(above, run[:, LANES:].astype(BF16))
        full = run[:, :LANES] + before - 1.0
        for i, m in enumerate(mine):
            rank = rank + jnp.where(m, full[i * blocks:(i + 1) * blocks, :], 0.0)
    pl.when(f < nf - 2)(enter)
    slot = owner.astype(jnp.float32) * cap + rank
    line = jnp.floor(slot * (1.0 / width))
    at = slot - line * width

    def wide(x):
        return jnp.broadcast_to(x, (16, LANES)).astype(BF16)

    def one_hot(x, count, payloads):
        picks = [x == ids[i] for i in range(count // 16)]
        return [jnp.concatenate([jnp.where(m, p, zero) for m in picks], axis=0) for p in payloads]

    lhs = []
    rhs = []
    for j in range(blocks):
        pick = [wide(x[j:j + 1, :]) for x in (line, at, place, col, values)]
        lhs.append(jnp.concatenate(one_hot(pick[0], slots, pick[2:]), axis=0))
        rhs.append(one_hot(pick[1], width, [one])[0])
    moved = dot(jnp.concatenate(lhs, axis=1), jnp.concatenate(rhs, axis=1), True)
    cells = moved[:slots] * WIDE + moved[slots:2 * slots]
    vals = moved[2 * slots:]
    for o in range(nf):
        for h in range(width // LANES):
            piece = (slice(o * lines, (o + 1) * lines), slice(h * LANES, (h + 1) * LANES))
            packed[o, h * lines:(h + 1) * lines, :] = cells[piece]
            packed[o, rows + h * lines:rows + (h + 1) * lines, :] = vals[piece]

    def send(to):
        return pltpu.make_async_remote_copy(
            src_ref=packed.at[to], dst_ref=got.at[f], send_sem=gsend, recv_sem=grecv.at[f],
            device_id={"files": to}, device_id_type=MESH)

    def receive(source):
        return pltpu.make_async_remote_copy(
            src_ref=packed.at[f], dst_ref=got.at[source], send_sem=gsend, recv_sem=grecv.at[source],
            device_id={"files": source}, device_id_type=MESH)

    def cross(to):
        return pltpu.make_async_remote_copy(
            src_ref=packed.at[to], dst_ref=got.at[nf + f % 2], send_sem=gsend, recv_sem=grecv.at[nf + f % 2],
            device_id={"files": to, "rep": flipped(r, 2, nr)}, device_id_type=MESH)

    for to in range(nf - 1):
        pl.when(to < f)(lambda to=to: send(to).start())
        if direct and to in CROSS_AFTER:
            pl.when(f >= top)(lambda to=to: cross(CROSS_AFTER.index(to)).start())

    def add_points(chunks, base, count):
        lhs = []
        rhs = []
        for chunk in chunks:
            cells = chunk[0:rows, :]
            row = jnp.floor(cells * (1.0 / WIDE))
            col = cells - row * WIDE
            if count < nr:
                row = row - (base * half).astype(jnp.float32)
            for j in range(rows):
                row16, col16, val16 = [wide(x[j:j + 1, :]) for x in (row, col, chunk[rows:, :])]
                lhs.append(one_hot(row16, count * half, [val16])[0])
                rhs.append(one_hot(col16, WIDE, [one])[0])
        total = dot(jnp.concatenate(lhs, axis=1), jnp.concatenate(rhs, axis=1), True)
        for q in range(count):
            block = total[q * half:(q + 1) * half, :]
            acc[base + q, 0] += block[:, :LANES]
            acc[base + q, 1] += block[:, LANES:]

    got[f] = packed[f]

    @pl.when(f % 2 == 0)
    def _():
        pl.semaphore_wait(fready.at[f // 2], 1)
        send(f + 1).start()

    for i in range(1, nf // 2):
        @pl.when(f // 2 + i < nf // 2)
        def _():
            pl.semaphore_wait(fready.at[f // 2 + i], 2)
            send((f // 2 + i) * 2).start()
            send((f // 2 + i) * 2 + 1).start()

    def arrived(k):
        source = f
        bit = 1
        while bit < nf:
            source = source + (1 - 2 * ((f // bit) % 2)) * bit * ((k // bit) % 2)
            bit *= 2
        pl.when(k > 0)(lambda: receive(source).wait_recv())
        return source

    def step(t, carry):
        k = 2 * t
        if nf == 8:
            k = sum(jnp.where((f // 2 == z) & (t == i), first, 0)
                    for z, order in enumerate(PAIRS) for i, first in enumerate(order))
        pair = [arrived(k), arrived(k + 1)]
        add_points([got[source] for source in pair], 0, nr)
        return carry

    lax.fori_loop(0, nf // 2 - (jnp.where(f < 2, 1, 0) if direct else 0), step, 0)

    pl.when(r < nr - 1)(functools.partial(pl.semaphore_wait, rready, nr - 1 - r))
    even = r % 2 == 0
    odd = r % 2 == 1
    sibling = flipped(r, 1, nr)
    firsts = range(2, nr, 2)
    seconds = range(3, nr, 2)

    def pass_on(src, dst, i, to):
        return pltpu.make_async_remote_copy(
            src_ref=src, dst_ref=dst, send_sem=rsend.at[i], recv_sem=rrecv.at[i],
            device_id={"rep": to}, device_id_type=MESH)

    def across(k):
        return pass_on(acc.at[flipped(r, k, nr)], parts.at[k], k, flipped(r, k, nr))

    def aside(k):
        return pass_on(acc.at[flipped(r, k + 1, nr)], side.at[k // 2 - 1], nr + k // 2 - 1, sibling)

    def joined(k):
        return pass_on(side.at[k // 2 - 1], parts.at[k], k, flipped(r, k, nr))

    def join():
        @pl.when(odd)
        def _():
            for k in firsts:
                aside(k).wait_recv()
                side[k // 2 - 1] += acc[flipped(r, k, nr)]
                joined(k).start()

    @pl.when(even)
    def _():
        for k in firsts:
            across(k).start()
            aside(k).start()

    @pl.when(odd)
    def _():
        for k in seconds:
            across(k).start()
            parts[k] = jnp.zeros((2, half, LANES), jnp.float32)

    if direct:
        def late(t, carry):
            pl.when(t == 1)(join)
            pair = [top + 2 * t, top + 2 * t + 1]
            for source in pair:
                pltpu.make_async_remote_copy(
                    src_ref=packed.at[f], dst_ref=got.at[source], send_sem=gsend, recv_sem=grecv.at[source],
                    device_id={"files": (f + 1) % nf}, device_id_type=MESH).wait_recv()
            add_points([got[source] for source in pair], (r // 2) * 2, 2)
            return carry

        lax.fori_loop(0, jnp.where(f < 2, 2, 0), late, 0)
        pl.when(f >= 2)(join)
    else:
        join()
    across(1).start()
    parts[0] = acc[r]
    pltpu.make_async_remote_copy(
        src_ref=packed.at[pl.ds(0, nf - 1)], dst_ref=got.at[pl.ds(0, nf - 1)], send_sem=gsend, recv_sem=grecv.at[0],
        device_id={"files": f}, device_id_type=MESH).wait_send()
    if direct:
        @pl.when(f >= top)
        def _():
            pltpu.make_async_remote_copy(
                src_ref=packed.at[pl.ds(0, 2)], dst_ref=got.at[pl.ds(0, 2)], send_sem=gsend,
                recv_sem=grecv.at[0], device_id={"files": f}, device_id_type=MESH).wait_send()
    across(1).wait()
    for k in firsts:
        across(k).wait()

    @pl.when(even)
    def _():
        for k in firsts:
            aside(k).wait_send()
        for k in seconds:
            across(k).wait_recv()

    @pl.when(odd)
    def _():
        for k in seconds:
            across(k).wait_send()


def solution(mesh):
    nf = mesh.shape["files"]
    nr = mesh.shape["rep"]
    owned = TILES // nf
    quarter = TR // nr
    half = owned * quarter // 2

    def per_device(tile_id, pix_row, pix_col, point_value):
        points = tile_id.shape[0]
        cap = SLACK * points // nf
        shape = (points // LANES, LANES)
        message = 2 * cap // LANES
        out = pl.pallas_call(
            functools.partial(kernel, nf, nr, owned, quarter, cap),
            out_shape=jax.ShapeDtypeStruct((nr, 2, half, LANES), jnp.float32),
            in_specs=[pl.BlockSpec(memory_space=pl.ANY)] * 4,
            out_specs=pl.BlockSpec(memory_space=pltpu.VMEM),
            scratch_shapes=[
                pltpu.VMEM(shape, jnp.int32),
                pltpu.VMEM(shape, jnp.int32),
                pltpu.VMEM(shape, jnp.int32),
                pltpu.VMEM(shape, point_value.dtype),
                pltpu.VMEM((nf, message, LANES), jnp.float32),
                pltpu.VMEM((nf + 2, message, LANES), jnp.float32),
                pltpu.VMEM((nr, 2, half, LANES), jnp.float32),
                pltpu.VMEM((nr // 2 - 1, 2, half, LANES), jnp.float32),
                pltpu.SemaphoreType.REGULAR((nf // 2,)),
                pltpu.SemaphoreType.REGULAR,
                pltpu.SemaphoreType.DMA,
                pltpu.SemaphoreType.DMA((nf + 2,)),
                pltpu.SemaphoreType.DMA((nr + nr // 2 - 1,)),
                pltpu.SemaphoreType.DMA((nr + nr // 2 - 1,)),
            ],
            compiler_params=pltpu.CompilerParams(collective_id=0, has_side_effects=True,
                                                 vmem_limit_bytes=16 * 1024 * 1024),
        )(*[pltpu.with_memory_space_constraint(x.reshape(shape), pltpu.HBM)
            for x in (tile_id, pix_row, pix_col, point_value)])
        return jnp.sum(out, axis=0).reshape(owned, quarter, LANES)

    both = P(("files", "rep"))
    return jax.shard_map(per_device, mesh=mesh, in_specs=(both,) * 4,
                         out_specs=P("files", "rep", None), check_vma=False)
```

```python
import functools

import jax
import jax.numpy as jnp
from jax import lax
from jax.experimental import pallas as pl
from jax.experimental.pallas import tpu as pltpu
from jax.sharding import PartitionSpec as P

LANES = 128
WIDE = 256
TR = 32
TILES = 128
SLACK = 4
CROSS_AFTER = (1, 5)
EARLY = (0, 2, 1, 3)
PAIRS = ((0, 2, 4, 6), (0, 2, 6, 4), (0, 6, 2, 4), (0, 2, 4, 6))
MESH = pl.DeviceIdType.MESH
BF16 = jnp.bfloat16


def flipped(index, mask, count):
    out = index
    bit = 1
    while bit < count:
        if mask & bit:
            out = out + (1 - 2 * ((index // bit) % 2)) * bit
        bit *= 2
    return out


def iota(shape, dim):
    return lax.broadcasted_iota(jnp.int32, shape, dim)


def dot(a, b, transposed=False):
    return lax.dot_general(a, b, (((1,), (1 if transposed else 0,)), ((), ())),
                           preferred_element_type=jnp.float32)


def kernel(nf, nr, owned, quarter, cap, tile_ref, row_ref, col_ref, val_ref, parts,
           tile_in, row_in, col_in, val_in, packed, got, acc, side,
           fready, rready, gsend, grecv, rsend, rrecv):
    f = lax.axis_index("files")
    r = lax.axis_index("rep")
    half = owned * quarter // 2
    band = nr * half
    direct = nf == 8 and nr == 4
    top = nf - 2
    blocks = tile_ref.shape[0]
    width = min(WIDE, cap)
    lines = cap // width
    slots = nf * lines
    rows = cap // LANES

    loads = []
    for i, (src, dst) in enumerate(((tile_ref, tile_in), (row_ref, row_in), (col_ref, col_in), (val_ref, val_in))):
        load = pltpu.make_async_copy(src, dst, rsend.at[i])
        load.start()
        loads.append(load)
    barrier = pltpu.get_barrier_semaphore()

    def signal(sem, axis, to):
        pl.semaphore_signal(sem, inc=1, device_id={axis: to}, device_id_type=MESH)

    for i in range(1, nf):
        pl.when(f + i < nf)(functools.partial(signal, barrier, "files", f + i))
    for i in range(1, nr):
        pl.when(r + i < nr)(functools.partial(signal, barrier, "rep", r + i))
    if direct:
        @pl.when(f < 2)
        def _():
            for to in (top, top + 1):
                pl.semaphore_signal(barrier, inc=1, device_id={"files": to, "rep": flipped(r, 2, nr)},
                                    device_id_type=MESH)
    entered = f + r + (jnp.where(f >= top, 2, 0) if direct else 0)

    def enter():
        pl.when(entered > 0)(functools.partial(pl.semaphore_wait, barrier, entered))
        for i in range(1, nf):
            pl.when(f - i >= 0)(functools.partial(signal, fready.at[f // 2], "files", f - i))
        for i in range(1, nr):
            pl.when(r - i >= 0)(functools.partial(signal, rready, "rep", r - i))

    pl.when(f >= nf - 2)(enter)

    one = jnp.ones((), BF16)
    zero = jnp.zeros((), BF16)
    ids = [(iota((16, LANES), 0) + 16 * i).astype(jnp.float32).astype(BF16) for i in range(WIDE // 16)]
    upto = jnp.where(iota((LANES, 2 * LANES), 0) <= iota((LANES, 2 * LANES), 1), 1.0, 0.0).astype(BF16)
    group = max(1, WIDE // blocks)
    span = group * blocks
    i0 = iota((span, span), 0)
    i1 = iota((span, span), 1)
    above = jnp.where((i1 < i0) & (i1 // blocks == i0 // blocks), 1.0, 0.0).astype(BF16)
    acc[...] = jnp.zeros_like(acc)

    for load in loads:
        load.wait()
    tile = tile_in[...]
    prow = row_in[...]
    owner = tile % nf
    inner = (tile // nf) * quarter + prow % quarter
    place = ((prow // quarter) * half + inner % half).astype(jnp.float32)
    col = ((inner // half) * LANES + col_in[...]).astype(jnp.float32)
    values = val_in[...].astype(jnp.float32)

    rank = jnp.zeros((blocks, LANES), jnp.float32)
    for g in range(0, nf, group):
        mine = [owner == o for o in range(g, g + group)]
        marks = jnp.concatenate([jnp.where(m, 1.0, 0.0) for m in mine], axis=0).astype(BF16)
        run = dot(marks, upto)
        before = dot(above, run[:, LANES:].astype(BF16))
        full = run[:, :LANES] + before - 1.0
        for i, m in enumerate(mine):
            rank = rank + jnp.where(m, full[i * blocks:(i + 1) * blocks, :], 0.0)
    pl.when(f < nf - 2)(enter)
    slot = owner.astype(jnp.float32) * cap + rank
    line = jnp.floor(slot * (1.0 / width))
    at = slot - line * width

    def wide(x):
        return jnp.broadcast_to(x, (16, LANES)).astype(BF16)

    def one_hot(x, count, payloads):
        picks = [x == ids[i] for i in range(count // 16)]
        return [jnp.concatenate([jnp.where(m, p, zero) for m in picks], axis=0) for p in payloads]

    lhs = []
    rhs = []
    for j in range(blocks):
        pick = [wide(x[j:j + 1, :]) for x in (line, at, place, col, values)]
        lhs.append(jnp.concatenate(one_hot(pick[0], slots, pick[2:]), axis=0))
        rhs.append(one_hot(pick[1], width, [one])[0])
    moved = dot(jnp.concatenate(lhs, axis=1), jnp.concatenate(rhs, axis=1), True)
    cells = moved[:slots] * WIDE + moved[slots:2 * slots]
    vals = moved[2 * slots:]
    for o in range(nf):
        for h in range(width // LANES):
            piece = (slice(o * lines, (o + 1) * lines), slice(h * LANES, (h + 1) * LANES))
            packed[o, h * lines:(h + 1) * lines, :] = cells[piece]
            packed[o, rows + h * lines:rows + (h + 1) * lines, :] = vals[piece]

    def send(to):
        return pltpu.make_async_remote_copy(
            src_ref=packed.at[to], dst_ref=got.at[f], send_sem=gsend, recv_sem=grecv.at[f],
            device_id={"files": to}, device_id_type=MESH)

    def receive(source):
        return pltpu.make_async_remote_copy(
            src_ref=packed.at[f], dst_ref=got.at[source], send_sem=gsend, recv_sem=grecv.at[source],
            device_id={"files": source}, device_id_type=MESH)

    def cross(to):
        return pltpu.make_async_remote_copy(
            src_ref=packed.at[to], dst_ref=got.at[nf + f % 2], send_sem=gsend, recv_sem=grecv.at[nf + f % 2],
            device_id={"files": to, "rep": flipped(r, 2, nr)}, device_id_type=MESH)

    for to in range(nf - 1):
        turn = jnp.where(f >= 4, EARLY[to], to) if direct and to < 4 else to
        pl.when(turn < f)(lambda turn=turn: send(turn).start())
        if direct and to in CROSS_AFTER:
            pl.when(f >= top)(lambda to=to: cross(CROSS_AFTER.index(to)).start())

    def add_points(chunks, base, count):
        lhs = []
        rhs = []
        for chunk in chunks:
            cells = chunk[0:rows, :]
            row = jnp.floor(cells * (1.0 / WIDE))
            col = cells - row * WIDE
            if count < nr:
                row = row - (base * half).astype(jnp.float32)
            for j in range(rows):
                row16, col16, val16 = [wide(x[j:j + 1, :]) for x in (row, col, chunk[rows:, :])]
                lhs.append(one_hot(row16, count * half, [val16])[0])
                rhs.append(one_hot(col16, WIDE, [one])[0])
        total = dot(jnp.concatenate(lhs, axis=1), jnp.concatenate(rhs, axis=1), True)
        for q in range(count):
            block = total[q * half:(q + 1) * half, :]
            acc[base + q, 0] += block[:, :LANES]
            acc[base + q, 1] += block[:, LANES:]

    got[f] = packed[f]

    @pl.when(f % 2 == 0)
    def _():
        pl.semaphore_wait(fready.at[f // 2], 1)
        send(f + 1).start()

    for i in range(1, nf // 2):
        @pl.when(f // 2 + i < nf // 2)
        def _():
            pl.semaphore_wait(fready.at[f // 2 + i], 2)
            send((f // 2 + i) * 2).start()
            send((f // 2 + i) * 2 + 1).start()

    def arrived(k):
        source = f
        bit = 1
        while bit < nf:
            source = source + (1 - 2 * ((f // bit) % 2)) * bit * ((k // bit) % 2)
            bit *= 2
        pl.when(k > 0)(lambda: receive(source).wait_recv())
        return source

    def step(t, carry):
        k = 2 * t
        if nf == 8:
            k = sum(jnp.where((f // 2 == z) & (t == i), first, 0)
                    for z, order in enumerate(PAIRS) for i, first in enumerate(order))
        pair = [arrived(k), arrived(k + 1)]
        add_points([got[source] for source in pair], 0, nr)
        return carry

    lax.fori_loop(0, nf // 2 - (jnp.where(f < 2, 1, 0) if direct else 0), step, 0)

    pl.when(r < nr - 1)(functools.partial(pl.semaphore_wait, rready, nr - 1 - r))
    even = r % 2 == 0
    odd = r % 2 == 1
    sibling = flipped(r, 1, nr)
    firsts = range(2, nr, 2)
    seconds = range(3, nr, 2)

    def pass_on(src, dst, i, to):
        return pltpu.make_async_remote_copy(
            src_ref=src, dst_ref=dst, send_sem=rsend.at[i], recv_sem=rrecv.at[i],
            device_id={"rep": to}, device_id_type=MESH)

    def across(k):
        return pass_on(acc.at[flipped(r, k, nr)], parts.at[k], k, flipped(r, k, nr))

    def aside(k):
        return pass_on(acc.at[flipped(r, k + 1, nr)], side.at[k // 2 - 1], nr + k // 2 - 1, sibling)

    def joined(k):
        return pass_on(side.at[k // 2 - 1], parts.at[k], k, flipped(r, k, nr))

    def join():
        @pl.when(odd)
        def _():
            for k in firsts:
                aside(k).wait_recv()
                side[k // 2 - 1] += acc[flipped(r, k, nr)]
                joined(k).start()

    @pl.when(even)
    def _():
        for k in firsts:
            across(k).start()
            aside(k).start()

    @pl.when(odd)
    def _():
        for k in seconds:
            across(k).start()
            parts[k] = jnp.zeros((2, half, LANES), jnp.float32)

    if direct:
        def late(t, carry):
            pl.when(t == 1)(join)
            pair = [top + 2 * t, top + 2 * t + 1]
            for source in pair:
                pltpu.make_async_remote_copy(
                    src_ref=packed.at[f], dst_ref=got.at[source], send_sem=gsend, recv_sem=grecv.at[source],
                    device_id={"files": (f + 1) % nf}, device_id_type=MESH).wait_recv()
            add_points([got[source] for source in pair], (r // 2) * 2, 2)
            return carry

        lax.fori_loop(0, jnp.where(f < 2, 2, 0), late, 0)
        pl.when(f >= 2)(join)
    else:
        join()
    across(1).start()
    parts[0] = acc[r]
    pltpu.make_async_remote_copy(
        src_ref=packed.at[pl.ds(0, nf - 1)], dst_ref=got.at[pl.ds(0, nf - 1)], send_sem=gsend, recv_sem=grecv.at[0],
        device_id={"files": f}, device_id_type=MESH).wait_send()
    if direct:
        @pl.when(f >= top)
        def _():
            pltpu.make_async_remote_copy(
                src_ref=packed.at[pl.ds(0, 2)], dst_ref=got.at[pl.ds(0, 2)], send_sem=gsend,
                recv_sem=grecv.at[0], device_id={"files": f}, device_id_type=MESH).wait_send()
    across(1).wait()
    for k in firsts:
        across(k).wait()

    @pl.when(even)
    def _():
        for k in firsts:
            aside(k).wait_send()
        for k in seconds:
            across(k).wait_recv()

    @pl.when(odd)
    def _():
        for k in seconds:
            across(k).wait_send()


def solution(mesh):
    nf = mesh.shape["files"]
    nr = mesh.shape["rep"]
    owned = TILES // nf
    quarter = TR // nr
    half = owned * quarter // 2

    def per_device(tile_id, pix_row, pix_col, point_value):
        points = tile_id.shape[0]
        cap = SLACK * points // nf
        shape = (points // LANES, LANES)
        message = 2 * cap // LANES
        out = pl.pallas_call(
            functools.partial(kernel, nf, nr, owned, quarter, cap),
            out_shape=jax.ShapeDtypeStruct((nr, 2, half, LANES), jnp.float32),
            in_specs=[pl.BlockSpec(memory_space=pl.ANY)] * 4,
            out_specs=pl.BlockSpec(memory_space=pltpu.VMEM),
            scratch_shapes=[
                pltpu.VMEM(shape, jnp.int32),
                pltpu.VMEM(shape, jnp.int32),
                pltpu.VMEM(shape, jnp.int32),
                pltpu.VMEM(shape, point_value.dtype),
                pltpu.VMEM((nf, message, LANES), jnp.float32),
                pltpu.VMEM((nf + 2, message, LANES), jnp.float32),
                pltpu.VMEM((nr, 2, half, LANES), jnp.float32),
                pltpu.VMEM((nr // 2 - 1, 2, half, LANES), jnp.float32),
                pltpu.SemaphoreType.REGULAR((nf // 2,)),
                pltpu.SemaphoreType.REGULAR,
                pltpu.SemaphoreType.DMA,
                pltpu.SemaphoreType.DMA((nf + 2,)),
                pltpu.SemaphoreType.DMA((nr + nr // 2 - 1,)),
                pltpu.SemaphoreType.DMA((nr + nr // 2 - 1,)),
            ],
            compiler_params=pltpu.CompilerParams(collective_id=0, has_side_effects=True,
                                                 vmem_limit_bytes=16 * 1024 * 1024),
        )(*[pltpu.with_memory_space_constraint(x.reshape(shape), pltpu.HBM)
            for x in (tile_id, pix_row, pix_col, point_value)])
        return jnp.sum(out, axis=0).reshape(owned, quarter, LANES)

    both = P(("files", "rep"))
    return jax.shard_map(per_device, mesh=mesh, in_specs=(both,) * 4,
                         out_specs=P("files", "rep", None), check_vma=False)
```
